32 devices in a mesh: tm: 8 (over z, y), tensor: 4 (over x, core).
Axes of the slice: x: 2, y: 2, z: 4, core: 2. Of those that a mesh axis runs over, the one named last changes fastest.
Arguments:
- frames_in: bfloat16 [8, 528, 1024], P('tm'), may hold values from -6 to 6
- frame_time: int32 [8], replicated, may hold values from 0 to 7, each once
- cond_count: int32 [8], replicated, may hold values from 0 to 2
- ln1_gain: float32 [2, 1024], replicated, may hold values from 0.5 to 1.5
- ln1_bias: float32 [2, 1024], replicated, may hold values from -1.75 to 1.75
- qkv_weight: bfloat16 [2, 3, 1024, 1024], P(None, None, None, 'tensor'), may hold values from -17 to 17
- qkv_bias: float32 [2, 3, 1024], P(None, None, 'tensor'), may hold values from -1.75 to 1.75
- out_weight: bfloat16 [2, 1024, 1024], P(None, 'tensor'), may hold values from -0.1875 to 0.1875
- out_bias: float32 [2, 1024], replicated, may hold values from -1.75 to 1.75
- ln2_gain: float32 [2, 1024], replicated, may hold values from 0.5 to 1.5
- ln2_bias: float32 [2, 1024], replicated, may hold values from -1.75 to 1.75
- fc1_weight: bfloat16 [2, 1024, 4096], P(None, None, 'tensor'), may hold values from -0.1875 to 0.1875
- fc1_bias: float32 [2, 4096], P(None, 'tensor'), may hold values from -3 to 3
- fc2_weight: bfloat16 [2, 4096, 1024], P(None, 'tensor'), may hold values from -0.09375 to 0.09375
- fc2_bias: float32 [2, 1024], replicated, may hold values from -1.75 to 1.75
Outputs:
- frames_out: bfloat16 [8, 528, 1024], P('tm', 'tensor')
The draws below stay inside these ranges and needn't reach their ends.
Inputs may be any that keep to these rules, and one draw needn't show every extreme that they name: `frame_time`: every time index 0 to 7 appears once. `cond_count`: the valid action and state tokens of a frame are its first ones.
All inputs are finite; a program needn't handle non-finite values.
Results may differ from the reference program's by a relative error of at most 0.04.
Values may be sent and summed in bfloat16 or wider, within the bound.
A program may use at most 128 MiB of HBM per device.

```python
import jax
import jax.numpy as jnp
from jax import lax

D = 1024
HEADS = 16
FF = 4096
PATCH_DEV = 64
COND = 2
SEQS = 8
LAYERS = 2
FRAMES = 8
ROWS = 528
N_TM = 8


def draw_qkv_weight(key, part):
    weights_raw = jnp.clip(jax.random.normal(jax.random.fold_in(key, 101), (LAYERS, 3, D, D), jnp.float32), -5.0, 5.0) * D ** (-0.5)
    return weights_raw.astype(jnp.bfloat16)


def plant(values, stream_key, low, high):
    longest = values.shape.index(max(values.shape))
    spots = []
    for shift in (0, 1):
        where = [jax.random.randint(jax.random.fold_in(stream_key, axis), (), 0, length) for axis, length in enumerate(values.shape)]
        where[longest] = (where[longest] + shift) % values.shape[longest]
        spots.append(tuple(where))
    return values.at[spots[0]].set(low).at[spots[1]].set(high)


def shard_levels(rng, shape, cuts, low, largest):
    gain, own = 1.0, jax.random.fold_in(rng, 6)
    for dim, parts in cuts:
        draws = jnp.exp(jax.random.uniform(jax.random.fold_in(own, dim), (parts,), jnp.float32, low / len(cuts), largest / len(cuts)))
        gain = gain * jnp.repeat(draws, shape[dim] // parts).reshape([-1 if axis == dim else 1 for axis in range(len(shape))])
    return gain


def normal_values(rng, dims, scale, limit, split=(), kind=jnp.bfloat16):
    array = jax.random.normal(rng, dims, jnp.float32) * scale
    if len(split) > 0:
        array = shard_levels(rng, dims, split, -0.22, 0.18) * array
    return jnp.clip(array, min=-limit, max=limit).astype(kind)


def setup_inputs(seed: int = 0) -> dict:
    keys = jax.random.split(jax.random.key(seed), 16)
    return {
        "frames_in": normal_values(keys[0], (N_TM, ROWS, D), 1.0, 6.0, ((0, 8),)),
        "frame_time": jax.random.permutation(keys[1], FRAMES).astype(jnp.int32),
        "cond_count": plant(jax.random.randint(keys[2], (FRAMES,), 0, COND + 1), jax.random.fold_in(keys[2], 1), 0, COND).astype(jnp.int32),
        "ln1_gain": jnp.clip(1.0 + 0.1 * jax.random.normal(keys[3], (LAYERS, D), jnp.float32), 0.5, 1.5),
        "ln1_bias": normal_values(keys[4], (LAYERS, D), 0.3, 1.75, (), jnp.float32),
        "qkv_weight": draw_qkv_weight(jax.random.fold_in(keys[15], 71), 0),
        "qkv_bias": normal_values(keys[6], (LAYERS, 3, D), 0.3, 1.75, ((2, 4),), jnp.float32),
        "out_weight": normal_values(keys[7], (LAYERS, D, D), D ** -0.5, 0.1875, ((1, 4),)),
        "out_bias": normal_values(keys[8], (LAYERS, D), 0.3, 1.75, (), jnp.float32),
        "ln2_gain": jnp.clip(1.0 + 0.1 * jax.random.normal(keys[9], (LAYERS, D), jnp.float32), 0.5, 1.5),
        "ln2_bias": normal_values(keys[10], (LAYERS, D), 0.3, 1.75, (), jnp.float32),
        "fc1_weight": normal_values(keys[11], (LAYERS, D, FF), D ** -0.5, 0.1875, ((2, 4),)),
        "fc1_bias": normal_values(keys[12], (LAYERS, FF), 0.5, 3.0, ((1, 4),), jnp.float32),
        "fc2_weight": normal_values(keys[13], (LAYERS, FF, D), FF ** -0.5, 0.09375, ((1, 4),)),
        "fc2_bias": normal_values(keys[14], (LAYERS, D), 0.3, 1.75, (), jnp.float32),
    }


def layer_norm(inputs, gain_row, bias_row):
    center = lax.optimization_barrier(jnp.mean(inputs, axis=-1, keepdims=True))
    spread = lax.optimization_barrier(jnp.mean(jnp.square(inputs - center), axis=-1, keepdims=True))
    return (inputs - center) * lax.rsqrt(spread + 1e-06) * gain_row + bias_row

def piece_tables(frame_time, cond_count, piece_count, frame_split, piece_rows):
    cond_dev = COND // frame_split
    piece_ids = jnp.arange(piece_count, dtype=jnp.int32)
    frame_ids = jnp.arange(frame_time.shape[0], dtype=jnp.int32)
    matches = (piece_ids // frame_split)[:, None] == frame_ids[None, :]
    piece_time = lax.optimization_barrier(jnp.sum(jnp.where(matches, frame_time[None, :], 0), axis=1)).astype(jnp.int32)
    piece_cond = lax.optimization_barrier(jnp.sum(jnp.where(matches, cond_count[None, :], 0), axis=1)).astype(jnp.int32)
    slot_index = jnp.arange(piece_rows, dtype=jnp.int32)
    cond_slot = (piece_ids % frame_split)[:, None] * cond_dev + slot_index[None, :] - PATCH_DEV
    valid = (slot_index[None, :] < PATCH_DEV) | (cond_slot < piece_cond[:, None])
    return (piece_time, valid)

def reference(frames_in, frame_time, cond_count, ln1_gain, ln1_bias, qkv_weight, qkv_bias, out_weight, out_bias, ln2_gain, ln2_bias, fc1_weight, fc1_bias, fc2_weight, fc2_bias):
    frame_split = N_TM // FRAMES
    cond_dev = COND // frame_split
    piece_rows = PATCH_DEV + cond_dev
    piece_time, valid = piece_tables(frame_time, cond_count, N_TM, frame_split, piece_rows)
    head_dim = D // HEADS
    scale = head_dim ** (-0.5)
    stream = frames_in
    for layer_idx in range(LAYERS):
        flattened = stream.reshape(-1, D).astype(jnp.float32)
        normed = layer_norm(flattened, ln1_gain[layer_idx], ln1_bias[layer_idx]).astype(jnp.bfloat16)
        projected = []
        for part_idx in range(3):
            result = jnp.dot(normed, qkv_weight[layer_idx, part_idx], preferred_element_type=jnp.float32) + qkv_bias[layer_idx, part_idx]
            result = lax.optimization_barrier(result.astype(jnp.bfloat16))
            projected.append(result.astype(jnp.float32).reshape(N_TM, SEQS, piece_rows, HEADS, head_dim))
        queries, keys_all, values_all = projected

        def one_piece(piece_idx):
            query_block = lax.dynamic_index_in_dim(queries, piece_idx, 0, keepdims=False)
            scores = jnp.einsum('sqhd,gskhd->shqgk', query_block, keys_all) * scale
            my_time = lax.dynamic_index_in_dim(piece_time, piece_idx, 0, keepdims=False)
            allowed = (piece_time <= my_time)[:, None] & valid
            scores = jnp.where(allowed, scores, -1e+30)
            highest = lax.optimization_barrier(jnp.max(scores, axis=(3, 4), keepdims=True))
            weights = jnp.where(allowed, jnp.exp(scores - highest), 0.0)
            totals = lax.optimization_barrier(jnp.sum(weights, axis=(3, 4)))
            rounded = lax.optimization_barrier(weights.astype(jnp.bfloat16)).astype(jnp.float32)
            mixed = jnp.einsum('shqgk,gskhd->shqd', rounded, values_all) / totals[..., None]
            return jnp.transpose(mixed, (0, 2, 1, 3)).reshape(SEQS * piece_rows, D).astype(jnp.bfloat16)
        attended = lax.map(one_piece, jnp.arange(N_TM, dtype=jnp.int32))
        projection = jnp.dot(attended.reshape(-1, D), out_weight[layer_idx], preferred_element_type=jnp.float32)
        first = flattened + projection + out_bias[layer_idx]
        normed_two = layer_norm(first, ln2_gain[layer_idx], ln2_bias[layer_idx]).astype(jnp.bfloat16)
        inner = jax.nn.gelu(jnp.dot(normed_two, fc1_weight[layer_idx], preferred_element_type=jnp.float32) + fc1_bias[layer_idx], approximate=False).astype(jnp.bfloat16)
        output = jnp.dot(inner, fc2_weight[layer_idx], preferred_element_type=jnp.float32)
        stream = (first + output + fc2_bias[layer_idx]).astype(jnp.bfloat16).reshape(N_TM, SEQS * piece_rows, D)
    return stream
```

```python
import jax
import jax.numpy as jnp
from jax import lax
from jax.sharding import PartitionSpec as P

D = 1024
HEADS = 16
PATCH_DEV = 64
COND = 2
LAYERS = 2


def layer_norm(inputs, gain_row, bias_row):
    center = jnp.mean(inputs, axis=-1, keepdims=True)
    spread = jnp.mean(jnp.square(inputs - center), axis=-1, keepdims=True)
    return (inputs - center) * lax.rsqrt(spread + 1e-06) * gain_row + bias_row


def piece_tables(frame_time, cond_count, piece_count, frame_split, piece_rows):
    cond_dev = COND // frame_split
    piece_ids = jnp.arange(piece_count, dtype=jnp.int32)
    frame_ids = jnp.arange(frame_time.shape[0], dtype=jnp.int32)
    matches = (piece_ids // frame_split)[:, None] == frame_ids[None, :]
    piece_time = jnp.sum(jnp.where(matches, frame_time[None, :], 0), axis=1)
    piece_cond = jnp.sum(jnp.where(matches, cond_count[None, :], 0), axis=1)
    slot_index = jnp.arange(piece_rows, dtype=jnp.int32)
    cond_slot = (piece_ids % frame_split)[:, None] * cond_dev + slot_index[None, :] - PATCH_DEV
    valid = (slot_index[None, :] < PATCH_DEV) | (cond_slot < piece_cond[:, None])
    return (piece_time, valid)


def shards_gather(
    frames_in,
    frame_time,
    cond_count,
    ln1_gain,
    ln1_bias,
    qkv_weight,
    qkv_bias,
    out_weight,
    out_bias,
    ln2_gain,
    ln2_bias,
    fc1_weight,
    fc1_bias,
    fc2_weight,
    fc2_bias,
):
    frame_count = frame_time.shape[0]
    piece_count = lax.axis_size("tm")
    frame_split = piece_count // frame_count
    cond_dev = COND // frame_split
    piece_rows = PATCH_DEV + cond_dev
    row_count = frames_in.shape[1]
    seq_count = row_count // piece_rows
    head_dim = D // HEADS
    head_local = qkv_weight.shape[3] // head_dim
    scale = head_dim ** (-0.5)
    tensor_size = lax.axis_size("tensor")
    tensor_pos = lax.axis_index("tensor")
    my_piece = lax.axis_index("tm")
    share_rows = row_count // tensor_size
    piece_time, valid = piece_tables(frame_time, cond_count, piece_count, frame_split, piece_rows)
    piece_ids = jnp.arange(piece_count, dtype=jnp.int32)
    my_time = jnp.sum(jnp.where(piece_ids == my_piece, piece_time, 0))
    full_in = frames_in[0]
    new_share = None
    for layer_idx in range(LAYERS):
        normed = layer_norm(
            full_in.astype(jnp.float32), ln1_gain[layer_idx], ln1_bias[layer_idx]
        ).astype(jnp.bfloat16)
        projected = jnp.einsum(
            "rd,jde->jre", normed, qkv_weight[layer_idx], preferred_element_type=jnp.float32
        )
        projected = (projected + qkv_bias[layer_idx][:, None, :]).astype(jnp.bfloat16)
        queries = projected[0].reshape(seq_count, piece_rows, head_local, head_dim)
        keys_mine = projected[1].reshape(1, seq_count, piece_rows, head_local * head_dim)
        values_mine = projected[2].reshape(1, seq_count, piece_rows, head_local * head_dim)
        start_top = jnp.full((seq_count, head_local, piece_rows), -1e30, jnp.float32)
        key_block = lax.all_gather(keys_mine, "tm", axis=0, tiled=True)
        value_block = lax.all_gather(values_mine, "tm", axis=0, tiled=True)
        block_count = key_block.shape[0]
        block_ids = jnp.arange(block_count, dtype=jnp.int32)
        matches = block_ids[:, None] == piece_ids[None, :]
        key_time = jnp.sum(jnp.where(matches, piece_time[None, :], 0), axis=1)
        key_valid = jnp.any(matches[:, :, None] & valid[None, :, :], axis=1)
        allowed = (key_time <= my_time)[:, None] & key_valid
        top_run = start_top
        keys_split = key_block.reshape(block_count, seq_count, piece_rows, head_local, head_dim)
        values_split = value_block.reshape(block_count, seq_count, piece_rows, head_local, head_dim)
        scores = (
            jnp.einsum("sqhd,gskhd->shqgk", queries, keys_split, preferred_element_type=jnp.float32)
            * scale
        )
        scores = jnp.where(allowed, scores, -1e30)
        new_top = jnp.maximum(top_run, jnp.max(scores, axis=(3, 4)))
        weights = jnp.where(allowed, jnp.exp(scores - new_top[..., None, None]), 0.0)
        total_new = jnp.sum(weights, axis=(3, 4))
        mixed = jnp.einsum(
            "shqgk,gskhd->shqd",
            weights.astype(jnp.bfloat16),
            values_split,
            preferred_element_type=jnp.float32,
        )
        top_run = new_top
        attended = (
            (mixed / total_new[..., None])
            .transpose(0, 2, 1, 3)
            .reshape(row_count, head_local * head_dim)
            .astype(jnp.bfloat16)
        )
        out_layer = out_weight[layer_idx]
        fc1_layer = fc1_weight[layer_idx]
        fc2_layer = fc2_weight[layer_idx]
        fc1_layer_bias = fc1_bias[layer_idx]
        own_rows = lax.dynamic_slice_in_dim(full_in, tensor_pos * share_rows, share_rows, 0).astype(
            jnp.float32
        )
        first = (
            own_rows
            + lax.psum_scatter(
                jnp.dot(attended, out_layer, preferred_element_type=jnp.float32).astype(
                    jnp.bfloat16
                ),
                "tensor",
                scatter_dimension=0,
                tiled=True,
            ).astype(jnp.float32)
            + out_bias[layer_idx]
        )
        normed_two = layer_norm(first, ln2_gain[layer_idx], ln2_bias[layer_idx]).astype(
            jnp.bfloat16
        )
        inner = jax.nn.gelu(
            jnp.dot(
                lax.all_gather(normed_two, "tensor", axis=0, tiled=True),
                fc1_layer,
                preferred_element_type=jnp.float32,
            )
            + fc1_layer_bias,
            approximate=False,
        ).astype(jnp.bfloat16)
        mlp_share = lax.psum_scatter(
            jnp.dot(inner, fc2_layer, preferred_element_type=jnp.float32).astype(jnp.bfloat16),
            "tensor",
            scatter_dimension=0,
            tiled=True,
        ).astype(jnp.float32)
        new_share = (first + mlp_share + fc2_bias[layer_idx]).astype(jnp.bfloat16)
        if layer_idx + 1 < LAYERS:
            full_in = lax.all_gather(new_share, "tensor", axis=0, tiled=True)
    return new_share[None]


def shards_clip(
    frames_in,
    frame_time,
    cond_count,
    ln1_gain,
    ln1_bias,
    qkv_weight,
    qkv_bias,
    out_weight,
    out_bias,
    ln2_gain,
    ln2_bias,
    fc1_weight,
    fc1_bias,
    fc2_weight,
    fc2_bias,
):
    frame_count = frame_time.shape[0]
    piece_count = lax.axis_size("tm")
    frame_split = piece_count // frame_count
    piece_rows = PATCH_DEV + COND // frame_split
    row_count = frames_in.shape[1]
    seq_count = row_count // piece_rows
    clips = seq_count // piece_count
    head_dim = D // HEADS
    head_local = qkv_weight.shape[3] // head_dim
    scale = head_dim ** (-0.5)
    tensor_size = lax.axis_size("tensor")
    tensor_pos = lax.axis_index("tensor")
    share_rows = row_count // tensor_size
    share_cols = D // tensor_size
    piece_time, valid = piece_tables(frame_time, cond_count, piece_count, frame_split, piece_rows)
    row_time = jnp.repeat(piece_time, piece_rows)
    allowed = (row_time[None, :] <= row_time[:, None]) & valid.reshape(1, -1)
    clip_rows = piece_count * piece_rows
    mine = lax.dynamic_slice_in_dim(frames_in[0], tensor_pos * share_cols, share_cols, 1)
    mine = mine.reshape(piece_count, clips, piece_rows, share_cols)
    mine = lax.all_to_all(mine, "tm", 0, 0, tiled=True)
    mine = mine.transpose(1, 0, 2, 3).reshape(row_count, share_cols)
    full_in = lax.all_gather(mine, "tensor", axis=1, tiled=True)
    new_share = None
    for layer_idx in range(LAYERS):
        normed = layer_norm(
            full_in.astype(jnp.float32), ln1_gain[layer_idx], ln1_bias[layer_idx]
        ).astype(jnp.bfloat16)
        parts = []
        for i in range(3):
            part = jnp.dot(normed, qkv_weight[layer_idx, i], preferred_element_type=jnp.float32)
            part = (part + qkv_bias[layer_idx, i]).astype(jnp.bfloat16)
            parts.append(part.reshape(clips, clip_rows, head_local, head_dim))
        queries, keys, values = parts
        scores = (
            jnp.einsum("sqhd,skhd->shqk", queries, keys, preferred_element_type=jnp.float32) * scale
        )
        scores = jnp.where(allowed, scores, -1e30)
        top = jnp.max(scores, axis=-1, keepdims=True)
        weights = jnp.where(allowed, jnp.exp(scores - top), 0.0)
        total = jnp.sum(weights, axis=-1, keepdims=True)
        mixed = jnp.einsum(
            "shqk,skhd->shqd",
            weights.astype(jnp.bfloat16),
            values,
            preferred_element_type=jnp.float32,
        )
        attended = (
            (mixed / total)
            .transpose(0, 2, 1, 3)
            .reshape(row_count, head_local * head_dim)
            .astype(jnp.bfloat16)
        )
        own_rows = lax.dynamic_slice_in_dim(full_in, tensor_pos * share_rows, share_rows, 0).astype(
            jnp.float32
        )
        first = (
            own_rows
            + lax.psum_scatter(
                jnp.dot(
                    attended, out_weight[layer_idx], preferred_element_type=jnp.float32
                ).astype(jnp.bfloat16),
                "tensor",
                scatter_dimension=0,
                tiled=True,
            ).astype(jnp.float32)
            + out_bias[layer_idx]
        )
        normed_two = layer_norm(first, ln2_gain[layer_idx], ln2_bias[layer_idx]).astype(
            jnp.bfloat16
        )
        inner = jax.nn.gelu(
            jnp.dot(
                lax.all_gather(normed_two, "tensor", axis=0, tiled=True),
                fc1_weight[layer_idx],
                preferred_element_type=jnp.float32,
            )
            + fc1_bias[layer_idx],
            approximate=False,
        ).astype(jnp.bfloat16)
        mlp_share = lax.psum_scatter(
            jnp.dot(inner, fc2_weight[layer_idx], preferred_element_type=jnp.float32).astype(
                jnp.bfloat16
            ),
            "tensor",
            scatter_dimension=0,
            tiled=True,
        ).astype(jnp.float32)
        new_share = (first + mlp_share + fc2_bias[layer_idx]).astype(jnp.bfloat16)
        if layer_idx + 1 < LAYERS:
            full_in = lax.all_gather(new_share, "tensor", axis=0, tiled=True)
    cols = jnp.stack(jnp.split(new_share, tensor_size, axis=1))
    cols = lax.all_to_all(cols, "tensor", 0, 0, tiled=True)
    cols = cols.reshape(clips, piece_count, piece_rows, share_cols).transpose(1, 0, 2, 3)
    cols = lax.all_to_all(cols, "tm", 0, 0, tiled=True)
    cols = cols.reshape(tensor_size, share_rows, share_cols)
    cols = lax.all_to_all(cols, "tensor", 0, 0, tiled=True)
    out = cols.transpose(1, 0, 2).reshape(share_rows, D)
    return out[None]


def shards(frames_in, frame_time, cond_count, *rest):
    frame_split = lax.axis_size("tm") // frame_time.shape[0]
    piece_rows = PATCH_DEV + COND // frame_split
    seq_count = frames_in.shape[1] // piece_rows
    by_clip = seq_count % lax.axis_size("tm") == 0
    body = shards_clip if by_clip else shards_gather
    return body(frames_in, frame_time, cond_count, *rest)


def solution(mesh):
    in_specs = (
        P("tm", None, None),
        P(),
        P(),
        P(),
        P(),
        P(None, None, None, "tensor"),
        P(None, None, "tensor"),
        P(None, "tensor", None),
        P(),
        P(),
        P(),
        P(None, None, "tensor"),
        P(None, "tensor"),
        P(None, "tensor", None),
        P(),
    )
    out_specs = P("tm", "tensor", None)
    return jax.shard_map(shards, mesh=mesh, in_specs=in_specs, out_specs=out_specs, check_vma=False)
```

```python
import jax
import jax.numpy as jnp
from jax import lax
from jax.experimental import pallas as pl
from jax.experimental.pallas import tpu as pltpu
from jax.sharding import PartitionSpec as P

D = 1024
HEADS = 16
PATCH_DEV = 64
COND = 2
LAYERS = 2


def layer_norm(inputs, gain_row, bias_row):
    center = jnp.mean(inputs, axis=-1, keepdims=True)
    spread = jnp.mean(jnp.square(inputs - center), axis=-1, keepdims=True)
    return (inputs - center) * lax.rsqrt(spread + 1e-06) * gain_row + bias_row


def piece_tables(frame_time, cond_count, piece_count, frame_split, piece_rows):
    cond_dev = COND // frame_split
    piece_ids = jnp.arange(piece_count, dtype=jnp.int32)
    frame_ids = jnp.arange(frame_time.shape[0], dtype=jnp.int32)
    matches = (piece_ids // frame_split)[:, None] == frame_ids[None, :]
    piece_time = jnp.sum(jnp.where(matches, frame_time[None, :], 0), axis=1)
    piece_cond = jnp.sum(jnp.where(matches, cond_count[None, :], 0), axis=1)
    slot_index = jnp.arange(piece_rows, dtype=jnp.int32)
    cond_slot = (piece_ids % frame_split)[:, None] * cond_dev + slot_index[None, :] - PATCH_DEV
    valid = (slot_index[None, :] < PATCH_DEV) | (cond_slot < piece_cond[:, None])
    return (piece_time, valid)


def shards_gather(
    frames_in,
    frame_time,
    cond_count,
    ln1_gain,
    ln1_bias,
    qkv_weight,
    qkv_bias,
    out_weight,
    out_bias,
    ln2_gain,
    ln2_bias,
    fc1_weight,
    fc1_bias,
    fc2_weight,
    fc2_bias,
):
    frame_count = frame_time.shape[0]
    piece_count = lax.axis_size("tm")
    frame_split = piece_count // frame_count
    cond_dev = COND // frame_split
    piece_rows = PATCH_DEV + cond_dev
    row_count = frames_in.shape[1]
    seq_count = row_count // piece_rows
    head_dim = D // HEADS
    head_local = qkv_weight.shape[3] // head_dim
    scale = head_dim ** (-0.5)
    tensor_size = lax.axis_size("tensor")
    tensor_pos = lax.axis_index("tensor")
    my_piece = lax.axis_index("tm")
    share_rows = row_count // tensor_size
    piece_time, valid = piece_tables(frame_time, cond_count, piece_count, frame_split, piece_rows)
    piece_ids = jnp.arange(piece_count, dtype=jnp.int32)
    my_time = jnp.sum(jnp.where(piece_ids == my_piece, piece_time, 0))
    full_in = frames_in[0]
    new_share = None
    for layer_idx in range(LAYERS):
        normed = layer_norm(
            full_in.astype(jnp.float32), ln1_gain[layer_idx], ln1_bias[layer_idx]
        ).astype(jnp.bfloat16)
        projected = jnp.einsum(
            "rd,jde->jre", normed, qkv_weight[layer_idx], preferred_element_type=jnp.float32
        )
        projected = (projected + qkv_bias[layer_idx][:, None, :]).astype(jnp.bfloat16)
        queries = projected[0].reshape(seq_count, piece_rows, head_local, head_dim)
        keys_mine = projected[1].reshape(1, seq_count, piece_rows, head_local * head_dim)
        values_mine = projected[2].reshape(1, seq_count, piece_rows, head_local * head_dim)
        start_top = jnp.full((seq_count, head_local, piece_rows), -1e30, jnp.float32)
        key_block = lax.all_gather(keys_mine, "tm", axis=0, tiled=True)
        value_block = lax.all_gather(values_mine, "tm", axis=0, tiled=True)
        block_count = key_block.shape[0]
        block_ids = jnp.arange(block_count, dtype=jnp.int32)
        matches = block_ids[:, None] == piece_ids[None, :]
        key_time = jnp.sum(jnp.where(matches, piece_time[None, :], 0), axis=1)
        key_valid = jnp.any(matches[:, :, None] & valid[None, :, :], axis=1)
        allowed = (key_time <= my_time)[:, None] & key_valid
        top_run = start_top
        keys_split = key_block.reshape(block_count, seq_count, piece_rows, head_local, head_dim)
        values_split = value_block.reshape(block_count, seq_count, piece_rows, head_local, head_dim)
        scores = (
            jnp.einsum("sqhd,gskhd->shqgk", queries, keys_split, preferred_element_type=jnp.float32)
            * scale
        )
        scores = jnp.where(allowed, scores, -1e30)
        new_top = jnp.maximum(top_run, jnp.max(scores, axis=(3, 4)))
        weights = jnp.where(allowed, jnp.exp(scores - new_top[..., None, None]), 0.0)
        total_new = jnp.sum(weights, axis=(3, 4))
        mixed = jnp.einsum(
            "shqgk,gskhd->shqd",
            weights.astype(jnp.bfloat16),
            values_split,
            preferred_element_type=jnp.float32,
        )
        top_run = new_top
        attended = (
            (mixed / total_new[..., None])
            .transpose(0, 2, 1, 3)
            .reshape(row_count, head_local * head_dim)
            .astype(jnp.bfloat16)
        )
        out_layer = out_weight[layer_idx]
        fc1_layer = fc1_weight[layer_idx]
        fc2_layer = fc2_weight[layer_idx]
        fc1_layer_bias = fc1_bias[layer_idx]
        own_rows = lax.dynamic_slice_in_dim(full_in, tensor_pos * share_rows, share_rows, 0).astype(
            jnp.float32
        )
        first = (
            own_rows
            + lax.psum_scatter(
                jnp.dot(attended, out_layer, preferred_element_type=jnp.float32).astype(
                    jnp.bfloat16
                ),
                "tensor",
                scatter_dimension=0,
                tiled=True,
            ).astype(jnp.float32)
            + out_bias[layer_idx]
        )
        normed_two = layer_norm(first, ln2_gain[layer_idx], ln2_bias[layer_idx]).astype(
            jnp.bfloat16
        )
        inner = jax.nn.gelu(
            jnp.dot(
                lax.all_gather(normed_two, "tensor", axis=0, tiled=True),
                fc1_layer,
                preferred_element_type=jnp.float32,
            )
            + fc1_layer_bias,
            approximate=False,
        ).astype(jnp.bfloat16)
        mlp_share = lax.psum_scatter(
            jnp.dot(inner, fc2_layer, preferred_element_type=jnp.float32).astype(jnp.bfloat16),
            "tensor",
            scatter_dimension=0,
            tiled=True,
        ).astype(jnp.float32)
        new_share = (first + mlp_share + fc2_bias[layer_idx]).astype(jnp.bfloat16)
        if layer_idx + 1 < LAYERS:
            full_in = lax.all_gather(new_share, "tensor", axis=0, tiled=True)
    return new_share[None]


MESH = pl.DeviceIdType.MESH


def layers_kernel(
    share_ref, qt_ref, kt_ref, g1, b1, qkvb, ob, g2, b2, f1b, f2b, wqkv_h, wo_h, w1_h, w2_h,
    out_ref, wqkv, wo, w1, w2, ag1, ag2, qb, kb, vb, inner, xs, keep, keep_x, stage, rbuf,
    wsem, ssem, rsem,
):
    share = share_ref.shape[0]
    head_dim = D // HEADS
    width = qb.shape[1]
    head_local = width // head_dim
    me = lax.axis_index("tensor")
    partner = me + 1 - 2 * (me % 2)
    across = (me + 2) % 4
    diagonal = (partner + 2) % 4

    pairs = ((wqkv_h, wqkv), (wo_h, wo), (w1_h, w1), (w2_h, w2))

    def weight_copy(l, j):
        return pltpu.make_async_copy(pairs[j][0].at[l], pairs[j][1].at[l], wsem.at[l, j])

    for l in range(LAYERS):
        for j in range(4):
            weight_copy(l, j).start()

    barrier = pltpu.get_barrier_semaphore()
    for other in (partner, across, diagonal):
        pl.semaphore_signal(barrier, inc=1, device_id={"tensor": other}, device_id_type=MESH)
    pl.semaphore_wait(barrier, 3)

    def rows(s):
        return pl.ds(pl.multiple_of(s * share, 16), share)

    def send(src, dst, l, j, target):
        copy = pltpu.make_async_remote_copy(
            src_ref=src,
            dst_ref=dst,
            send_sem=ssem.at[l, j],
            recv_sem=rsem.at[l, j],
            device_id={"tensor": target},
            device_id_type=MESH,
        )
        copy.start()
        return copy

    def gather(buf, l, j, use):
        own = buf.at[l, rows(me)]
        to_x = send(own, own, l, j, across)
        to_p = send(own, own, l, j + 1, partner)
        use(0, me)
        to_p.wait_recv()
        use(1, partner)
        to_x.wait_recv()
        got = buf.at[l, rows(across)]
        fwd = send(got, got, l, j + 2, partner)
        use(2, across)
        fwd.wait_recv()
        use(3, diagonal)
        to_x.wait_send()
        to_p.wait_send()
        fwd.wait_send()

    def norm(x, gain, bias):
        return layer_norm(x, gain, bias).astype(jnp.bfloat16)

    lane = lax.broadcasted_iota(jnp.int32, (1, width), 1)

    def layer(l, carry):
        ag1[l, rows(me)] = norm(xs[...], g1[l], b1[l])
        weight_copy(l, 0).wait()

        def project(step, s):
            normed = ag1[l, rows(s)]
            for i, dst in enumerate((qb, kb, vb)):
                y = jnp.dot(normed, wqkv[l, i], preferred_element_type=jnp.float32) + qkvb[l, i]
                if i == 0:
                    y = y * head_dim ** (-0.5)
                dst[rows(s)] = y.astype(jnp.bfloat16)

        gather(ag1, l, 0, project)
        weight_copy(l, 1).wait()

        def attend(s):
            q = qb[rows(s)]
            allowed = kt_ref[...] <= qt_ref[rows(s)]
            acc = jnp.zeros((share, width), jnp.float32)
            for h in range(head_local):
                mine = (lane >= h * head_dim) & (lane < (h + 1) * head_dim)
                qm = q * jnp.where(mine, 1.0, 0.0).astype(jnp.bfloat16)
                sc = lax.dot_general(
                    qm, kb[...], (((1,), (1,)), ((), ())), preferred_element_type=jnp.float32
                )
                sc = jnp.where(allowed, sc, -1e30)
                w = jnp.exp(sc - jnp.max(sc, axis=-1, keepdims=True))
                total = jnp.sum(w, axis=-1, keepdims=True)
                pv = jnp.dot(w.astype(jnp.bfloat16), vb[...], preferred_element_type=jnp.float32)
                acc = jnp.where(mine, pv / total, acc)
            return jnp.dot(
                acc.astype(jnp.bfloat16), wo[l], preferred_element_type=jnp.float32
            )

        stage[0] = attend(diagonal).astype(jnp.bfloat16)
        c_f = send(stage.at[0], rbuf.at[l, 0], l, 3, partner)
        part = attend(across)
        c_f.wait_recv()
        stage[1] = (part + rbuf[l, 0].astype(jnp.float32)).astype(jnp.bfloat16)
        c_x = send(stage.at[1], rbuf.at[l, 1], l, 4, across)
        stage[2] = attend(partner).astype(jnp.bfloat16)
        c_p = send(stage.at[2], rbuf.at[l, 2], l, 5, partner)
        part = attend(me) + xs[...] + ob[l]
        c_p.wait_recv()
        part = part + rbuf[l, 2].astype(jnp.float32)
        c_x.wait_recv()
        first = part + rbuf[l, 1].astype(jnp.float32)
        xs[...] = first
        ag2[l, rows(me)] = norm(first, g2[l], b2[l])
        c_f.wait_send()
        c_x.wait_send()
        c_p.wait_send()
        weight_copy(l, 2).wait()
        weight_copy(l, 3).wait()

        def mlp(s):
            normed = ag2[l, rows(s)]
            tile = 256
            for n in range(w1.shape[2] // tile):
                at = pl.ds(n * tile, tile)
                y = jnp.dot(normed, w1[l, :, at], preferred_element_type=jnp.float32) + f1b[l, :, at]
                y = 0.5 * y * (1.0 + lax.erf(y * (0.5**0.5)))
                inner[:, at] = y.astype(jnp.bfloat16)
            return jnp.dot(inner[...], w2[l], preferred_element_type=jnp.float32)

        copies = []

        def feed(step, s):
            part = mlp(s)
            if step == 0:
                keep[...] = part
            elif step == 1:
                stage[2] = part.astype(jnp.bfloat16)
                copies.append(send(stage.at[2], rbuf.at[l, 5], l, 11, partner))
            elif step == 2:
                keep_x[...] = part
            else:
                stage[0] = part.astype(jnp.bfloat16)
                copies.append(send(stage.at[0], rbuf.at[l, 3], l, 9, partner))

        gather(ag2, l, 6, feed)
        c_p, c_f = copies
        c_f.wait_recv()
        stage[1] = (keep_x[...] + rbuf[l, 3].astype(jnp.float32)).astype(jnp.bfloat16)
        c_x = send(stage.at[1], rbuf.at[l, 4], l, 10, across)
        c_p.wait_recv()
        part = keep[...] + xs[...] + f2b[l] + rbuf[l, 5].astype(jnp.float32)
        c_x.wait_recv()
        new = (part + rbuf[l, 4].astype(jnp.float32)).astype(jnp.bfloat16)
        xs[...] = new.astype(jnp.float32)
        c_p.wait_send()
        c_f.wait_send()
        c_x.wait_send()
        return carry

    xs[...] = share_ref[...].astype(jnp.float32)
    lax.fori_loop(0, LAYERS, layer, 0)
    out_ref[...] = xs[...].astype(jnp.bfloat16)


def shards_clip(
    frames_in,
    frame_time,
    cond_count,
    ln1_gain,
    ln1_bias,
    qkv_weight,
    qkv_bias,
    out_weight,
    out_bias,
    ln2_gain,
    ln2_bias,
    fc1_weight,
    fc1_bias,
    fc2_weight,
    fc2_bias,
):
    piece_count = lax.axis_size("tm")
    frame_split = piece_count // frame_time.shape[0]
    piece_rows = PATCH_DEV + COND // frame_split
    row_count = frames_in.shape[1]
    width = qkv_weight.shape[3]
    hidden = fc1_weight.shape[2]
    tensor_size = lax.axis_size("tensor")
    tensor_pos = lax.axis_index("tensor")
    share_rows = row_count // tensor_size
    share_cols = D // tensor_size
    share_pad = -(-share_rows // 16) * 16
    all_rows = share_pad * tensor_size
    piece_time, valid = piece_tables(frame_time, cond_count, piece_count, frame_split, piece_rows)
    far = jnp.int32(1 << 30)
    row_time = jnp.repeat(piece_time, piece_rows).reshape(tensor_size, share_rows)
    key_time = jnp.where(valid.reshape(tensor_size, share_rows), row_time, far)
    pad = ((0, 0), (0, share_pad - share_rows))
    row_time = jnp.pad(row_time, pad, constant_values=1 << 29).reshape(all_rows, 1)
    key_time = jnp.pad(key_time, pad, constant_values=1 << 30).reshape(1, all_rows)
    cols = lax.dynamic_slice_in_dim(frames_in[0], tensor_pos * share_cols, share_cols, 1)
    cols = cols.reshape(piece_count, piece_rows, share_cols)
    cols = lax.all_to_all(cols, "tm", 0, 0, tiled=True)
    cols = cols.reshape(tensor_size, share_rows, share_cols)
    cols = lax.all_to_all(cols, "tensor", 0, 0, tiled=True)
    share = cols.transpose(1, 0, 2).reshape(share_rows, D)
    share = jnp.pad(share, ((0, share_pad - share_rows), (0, 0)))

    vmem = pl.BlockSpec(memory_space=pltpu.VMEM)
    hbm = pl.BlockSpec(memory_space=pl.ANY)
    bf16, f32 = jnp.bfloat16, jnp.float32
    new_share = pl.pallas_call(
        layers_kernel,
        out_shape=jax.ShapeDtypeStruct((share_pad, D), bf16),
        in_specs=[vmem] * 11 + [hbm] * 4,
        out_specs=vmem,
        scratch_shapes=[
            pltpu.VMEM(qkv_weight.shape, bf16),
            pltpu.VMEM(out_weight.shape, bf16),
            pltpu.VMEM(fc1_weight.shape, bf16),
            pltpu.VMEM(fc2_weight.shape, bf16),
            pltpu.VMEM((LAYERS, all_rows, D), bf16),
            pltpu.VMEM((LAYERS, all_rows, D), bf16),
            pltpu.VMEM((all_rows, width), bf16),
            pltpu.VMEM((all_rows, width), bf16),
            pltpu.VMEM((all_rows, width), bf16),
            pltpu.VMEM((share_pad, hidden), bf16),
            pltpu.VMEM((share_pad, D), f32),
            pltpu.VMEM((share_pad, D), f32),
            pltpu.VMEM((share_pad, D), f32),
            pltpu.VMEM((3, share_pad, D), bf16),
            pltpu.VMEM((LAYERS, 6, share_pad, D), bf16),
            pltpu.SemaphoreType.DMA((LAYERS, 4)),
            pltpu.SemaphoreType.DMA((LAYERS, 12)),
            pltpu.SemaphoreType.DMA((LAYERS, 12)),
        ],
        compiler_params=pltpu.CompilerParams(
            collective_id=0, has_side_effects=True, vmem_limit_bytes=60 * 1024 * 1024
        ),
    )(
        share,
        row_time,
        key_time,
        ln1_gain[:, None],
        ln1_bias[:, None],
        qkv_bias[:, :, None],
        out_bias[:, None],
        ln2_gain[:, None],
        ln2_bias[:, None],
        fc1_bias[:, None],
        fc2_bias[:, None],
        qkv_weight,
        out_weight,
        fc1_weight,
        fc2_weight,
    )
    new_share = new_share[:share_rows]
    cols = jnp.stack(jnp.split(new_share, tensor_size, axis=1))
    cols = lax.all_to_all(cols, "tensor", 0, 0, tiled=True)
    cols = cols.reshape(piece_count, piece_rows, share_cols)
    cols = lax.all_to_all(cols, "tm", 0, 0, tiled=True)
    cols = cols.reshape(tensor_size, share_rows, share_cols)
    cols = lax.all_to_all(cols, "tensor", 0, 0, tiled=True)
    return cols.transpose(1, 0, 2).reshape(1, share_rows, D)


def shards(frames_in, frame_time, cond_count, *rest):
    frame_split = lax.axis_size("tm") // frame_time.shape[0]
    piece_rows = PATCH_DEV + COND // frame_split
    seq_count = frames_in.shape[1] // piece_rows
    by_clip = seq_count == lax.axis_size("tm") and lax.axis_size("tensor") == 4
    body = shards_clip if by_clip else shards_gather
    return body(frames_in, frame_time, cond_count, *rest)


def solution(mesh):
    in_specs = (
        P("tm", None, None),
        P(),
        P(),
        P(),
        P(),
        P(None, None, None, "tensor"),
        P(None, None, "tensor"),
        P(None, "tensor", None),
        P(),
        P(),
        P(),
        P(None, None, "tensor"),
        P(None, "tensor"),
        P(None, "tensor", None),
        P(),
    )
    out_specs = P("tm", "tensor", None)
    return jax.shard_map(shards, mesh=mesh, in_specs=in_specs, out_specs=out_specs, check_vma=False)
```
